128 devices in a mesh: seq: 32 (over y, z_hi, x), head: 4 (over z_lo, core).
Axes of the slice: x: 4, y: 4, z: 4 (z_hi: 2, z_lo: 2; z = z_hi * 2 + z_lo), core: 2. Of those that a mesh axis runs over, the one named last changes fastest.
Arguments:
- hidden: bfloat16 [4096, 3072], P('seq'), may hold values from -6 to 6
- cotangent: bfloat16 [4096, 3072], P('seq'), may hold values from -6 to 6
- mod_scale: float32 [3072], replicated, may hold values from -0.5 to 0.5
- mod_shift: float32 [3072], replicated, may hold values from -3 to 3
- branch_gate: float32 [3072], replicated, may hold values from 0.3 to 1.5
- query_weight: bfloat16 [3072, 1536], P('seq', 'head'), may hold values from -0.108253175 to 0.108253175, as said below
- key_weight: bfloat16 [3072, 1536], P('seq', 'head'), may hold values from -0.108253175 to 0.108253175, as said below
- value_weight: bfloat16 [3072, 1536], P('seq', 'head'), may hold values from -0.109375 to 0.109375
- output_weight: bfloat16 [3072, 1536], P('seq', 'head'), may hold values from -0.15625 to 0.15625
- query_gain: float32 [1536], P('head'), may hold values from 0.7 to 6.3
- key_gain: float32 [1536], P('head'), may hold values from 0.7 to 6.3
Outputs:
- hidden_grad: bfloat16 [4096, 3072], P('seq')
- outproj_grad: float32 [3072, 1536], P('seq', 'head')
The draws below stay inside these ranges and needn't reach their ends.
Inputs may be any that keep to these rules, and one draw needn't show every extreme that they name: `query_weight`: entries of the query projection, of order 3072^-0.5. `key_weight`: entries of the key projection, of order 3072^-0.5.
All inputs are finite; a program needn't handle non-finite values.
Results may differ from the reference program's by a relative error of at most 0.028.
Values may be sent and summed in bfloat16 or wider, within the bound.
No kernel may reach another device: no remote copies, remote signals or barrier semaphores. Data moves between devices by JAX's collectives and lax.ppermute only.
A program may use at most 128 MiB of HBM per device.

```python
import math
import jax
import jax.numpy as jnp
from jax import lax

D = 3072
HEADS = 12
HEAD_DIM = 128
SEQ = 4096


def weight_base(key, salt):
    values = jax.random.normal(jax.random.fold_in(key, salt), (D, HEADS * HEAD_DIM), jnp.float32)
    return jnp.clip(values, -6.0, 6.0) / math.sqrt(D)


def draw_query_weight(key, part):
    return weight_base(key, 11).astype(jnp.bfloat16)


def draw_key_weight(key, part):
    return weight_base(key, 12).astype(jnp.bfloat16)


def gain_base(key, salt):
    jitter = jnp.exp(jax.random.uniform(jax.random.fold_in(key, salt), (HEADS, HEAD_DIM), jnp.float32, math.log(0.7), math.log(1.4)))
    return jitter.reshape(-1)


def draw_query_gain(key, part):
    return gain_base(key, 21)


def draw_key_gain(key, part):
    return gain_base(key, 22)


def raised(array, stream_key, source, target, parts, factor):
    owner, partner = [(jnp.arange(array.shape[position]) // (array.shape[position] // parts)).reshape([-1 if axis == position else 1 for axis in range(array.ndim)]) for position in (source, target)]
    chosen = jax.random.permutation(stream_key, parts)[partner]
    strong = (owner == chosen) | (owner == (partner + parts // 2) % parts)
    return jnp.where(strong, factor * array, array)


def block_levels(key, dims, cuts, smallest, largest):
    factor_of, own = 1.0, jax.random.fold_in(key, 6)
    for dim, blocks in cuts:
        steps = jnp.exp(jax.random.uniform(jax.random.fold_in(own, dim), (blocks,), jnp.float32, smallest / len(cuts), largest / len(cuts)))
        factor_of = factor_of * jnp.repeat(steps, dims[dim] // blocks).reshape([-1 if axis == dim else 1 for axis in range(len(dims))])
    return factor_of


def scatter_about(stream_key, shape, spread, most, pieces=(), kind=jnp.bfloat16):
    entries = jax.random.normal(stream_key, shape, jnp.float32) * spread
    if len(pieces) > 0:
        entries = block_levels(stream_key, shape, pieces, -0.22, 0.18) * entries
    return jnp.clip(entries, min=-most, max=most).astype(kind)


def bell_draw_with(own_key, shape, deviation, reach, split, heavy, kind=jnp.bfloat16):
    values = deviation * jax.random.normal(own_key, shape, jnp.float32)
    if split:
        values = values * block_levels(own_key, shape, split, -0.22, 0.18)
    return jnp.clip(raised(values, jax.random.fold_in(own_key, 3), *heavy), -reach, reach).astype(kind)


def setup_inputs(seed: int = 0) -> dict:
    arg_keys = jax.random.split(jax.random.key(seed), 12)
    hidden = scatter_about(arg_keys[0], (SEQ, D), 1.0, 6.0, ((0, 32),))
    cotangent = bell_draw_with(arg_keys[1], (SEQ, D), 1.0, 6.0, ((0, 32),), (0, 1, 32, 2.75))
    mod_scale = jnp.clip(jax.random.uniform(arg_keys[2], (D,), jnp.float32, -0.5, 0.5), -0.5, 0.5)
    mod_shift = scatter_about(arg_keys[3], (D,), 0.5, 3.0, (), jnp.float32)
    branch_gate = jnp.clip(jax.random.uniform(arg_keys[4], (D,), jnp.float32, 0.3, 1.5), 0.3, 1.5)
    query_weight = draw_query_weight(jax.random.fold_in(arg_keys[11], 71), 0)
    key_weight = draw_key_weight(jax.random.fold_in(arg_keys[11], 71), 0)
    value_weight = scatter_about(arg_keys[7], (D, HEADS * HEAD_DIM), D ** -0.5, 0.109375, ((0, 32), (1, 4)))
    output_weight = scatter_about(arg_keys[8], (D, HEADS * HEAD_DIM), (HEADS * HEAD_DIM) ** -0.5, 0.15625, ((0, 32), (1, 4)))
    query_gain = draw_query_gain(jax.random.fold_in(arg_keys[11], 71), 0)
    key_gain = draw_key_gain(jax.random.fold_in(arg_keys[11], 71), 0)
    return dict(hidden=hidden, cotangent=cotangent, mod_scale=mod_scale, mod_shift=mod_shift, branch_gate=branch_gate, query_weight=query_weight, key_weight=key_weight, value_weight=value_weight, output_weight=output_weight, query_gain=query_gain, key_gain=key_gain)


EPSILON = 1e-06

def layer_normed(hidden, mod_scale, mod_shift):
    values = hidden.astype(jnp.float32)
    center = values - lax.optimization_barrier(jnp.mean(values, axis=-1, keepdims=True))
    inverse = lax.rsqrt(lax.optimization_barrier(jnp.mean(center * center, axis=-1, keepdims=True)) + EPSILON)
    unit = center * inverse
    normed = (unit * (1.0 + mod_scale) + mod_shift).astype(jnp.bfloat16)
    return (unit, inverse, normed)

def layer_back(grad, unit, inverse, mod_scale):
    scaled = grad * (1.0 + mod_scale)
    middle = lax.optimization_barrier(jnp.mean(scaled, axis=-1, keepdims=True))
    along = lax.optimization_barrier(jnp.mean(scaled * unit, axis=-1, keepdims=True))
    return inverse * (scaled - middle - unit * along)

def head_norm(raw, gain, factor):
    inverse = lax.rsqrt(lax.optimization_barrier(jnp.mean(raw * raw, axis=-1, keepdims=True)) + EPSILON)
    unit = raw * inverse
    return (unit, inverse, (unit * gain * factor).astype(jnp.bfloat16))

def head_back(grad, unit, inverse, gain, factor):
    scaled = grad * gain * factor
    along = lax.optimization_barrier(jnp.mean(scaled * unit, axis=-1, keepdims=True))
    return (inverse * (scaled - unit * along)).astype(jnp.bfloat16)

def reference(hidden, cotangent, mod_scale, mod_shift, branch_gate, query_weight, key_weight, value_weight, output_weight, query_gain, key_gain):
    factor = jnp.float32(1.0 / math.sqrt(HEAD_DIM))
    rows = hidden.shape[0]
    width = HEADS * HEAD_DIM
    cube = (rows, HEADS, HEAD_DIM)
    unit, inverse, normed = layer_normed(hidden, mod_scale, mod_shift)
    query_raw = jnp.dot(normed, query_weight, preferred_element_type=jnp.float32).reshape(cube)
    key_raw = jnp.dot(normed, key_weight, preferred_element_type=jnp.float32).reshape(cube)
    value_raw = jnp.dot(normed, value_weight, preferred_element_type=jnp.float32).reshape(cube)
    query_unit, query_inverse, query = head_norm(query_raw, query_gain.reshape(HEADS, HEAD_DIM), factor)
    key_unit, key_inverse, keys = head_norm(key_raw, key_gain.reshape(HEADS, HEAD_DIM), jnp.float32(1.0))
    values = value_raw.astype(jnp.bfloat16)
    keys_wide = keys.astype(jnp.float32)
    values_wide = values.astype(jnp.float32)
    block = math.gcd(rows, 512)
    count = rows // block

    def forward_block(query_block):
        scores = jnp.einsum('qhd,khd->hqk', query_block.astype(jnp.float32), keys_wide)
        top = lax.optimization_barrier(jnp.max(scores, axis=-1, keepdims=True))
        expo = jnp.exp(scores - top)
        total = lax.optimization_barrier(jnp.sum(expo, axis=-1, keepdims=True))
        probs = expo.astype(jnp.bfloat16).astype(jnp.float32)
        mixed = jnp.einsum('hqk,khd->hqd', probs, values_wide) / total
        mix = jnp.transpose(mixed, (1, 0, 2)).astype(jnp.bfloat16)
        log_total = jnp.transpose((top + jnp.log(total))[:, :, 0])
        return (mix, log_total)
    mix, log_total = lax.map(forward_block, query.reshape(count, block, HEADS, HEAD_DIM))
    mix = mix.reshape(cube)
    log_total = log_total.reshape(rows, HEADS)
    branch_cot = (cotangent.astype(jnp.float32) * branch_gate).astype(jnp.bfloat16)
    mix_flat = mix.reshape(rows, width)
    outproj_grad = jnp.dot(branch_cot.T, mix_flat, preferred_element_type=jnp.float32)
    mix_grad = jnp.dot(branch_cot, output_weight, preferred_element_type=jnp.float32).astype(jnp.bfloat16).reshape(cube)
    delta = lax.optimization_barrier(jnp.sum(mix_grad.astype(jnp.float32) * mix.astype(jnp.float32), axis=-1))

    def backward_block(carry, inputs):
        key_grad, value_grad = carry
        query_block, grad_block, log_block, delta_block = inputs
        query_wide = query_block.astype(jnp.float32)
        grad_wide = grad_block.astype(jnp.float32)
        scores = jnp.einsum('qhd,khd->hqk', query_wide, keys_wide)
        probs = jnp.exp(scores - jnp.transpose(log_block)[:, :, None])
        prob_grad = jnp.einsum('qhd,khd->hqk', grad_wide, values_wide)
        score_grad = (probs * (prob_grad - jnp.transpose(delta_block)[:, :, None])).astype(jnp.bfloat16).astype(jnp.float32)
        query_grad = jnp.einsum('hqk,khd->qhd', score_grad, keys_wide)
        key_grad = key_grad + jnp.einsum('hqk,qhd->khd', score_grad, query_wide)
        probs_low = probs.astype(jnp.bfloat16).astype(jnp.float32)
        value_grad = value_grad + jnp.einsum('hqk,qhd->khd', probs_low, grad_wide)
        return ((key_grad, value_grad), query_grad)
    zeros = jnp.zeros(cube, jnp.float32)
    inputs = (query.reshape(count, block, HEADS, HEAD_DIM), mix_grad.reshape(count, block, HEADS, HEAD_DIM), log_total.reshape(count, block, HEADS), delta.reshape(count, block, HEADS))
    (key_grad, value_grad), query_grad = lax.scan(backward_block, (zeros, zeros), inputs)
    query_grad = query_grad.reshape(cube)
    query_raw_grad = head_back(query_grad, query_unit, query_inverse, query_gain.reshape(HEADS, HEAD_DIM), factor).reshape(rows, width)
    key_raw_grad = head_back(key_grad, key_unit, key_inverse, key_gain.reshape(HEADS, HEAD_DIM), jnp.float32(1.0)).reshape(rows, width)
    value_raw_grad = value_grad.astype(jnp.bfloat16).reshape(rows, width)
    normed_grad = jnp.dot(query_raw_grad, query_weight.T, preferred_element_type=jnp.float32)
    normed_grad = normed_grad + jnp.dot(key_raw_grad, key_weight.T, preferred_element_type=jnp.float32)
    normed_grad = normed_grad + jnp.dot(value_raw_grad, value_weight.T, preferred_element_type=jnp.float32)
    hidden_grad = layer_back(normed_grad, unit, inverse, mod_scale).astype(jnp.bfloat16)
    return (hidden_grad, outproj_grad)
```

```python
import math

import jax
import jax.numpy as jnp
from jax import lax
from jax.experimental import pallas as pl
from jax.experimental.pallas import tpu as pltpu
from jax.sharding import Mesh
from jax.sharding import PartitionSpec as P

HEAD_DIM = 128
SEQ = ("y", "z", "x")
EPSILON = 1e-06
FACTOR = 1.0 / math.sqrt(HEAD_DIM)
ROLES = 4
GRAD_ROLE = 3
TILE = 256
F32 = jnp.float32
BF16 = jnp.bfloat16


def nt(a, b):
    return lax.dot_general(a, b, (((1,), (1,)), ((), ())), preferred_element_type=F32)


def nn(a, b):
    return lax.dot_general(a, b, (((1,), (0,)), ((), ())), preferred_element_type=F32)


def shifted(array, axis, shift, sources=None):
    peers = lax.axis_size(axis)
    sources = range(peers) if sources is None else sources
    return lax.ppermute(array, axis, [(i, (i + shift) % peers) for i in sources])


def call(kernel, outs, scratch=(), scalars=1):
    def run(*args):
        specs = [pl.BlockSpec(memory_space=pltpu.SMEM)] * scalars
        specs += [pl.BlockSpec(memory_space=pltpu.VMEM)] * (len(args) - scalars)
        return pl.pallas_call(
            kernel,
            out_shape=tuple(jax.ShapeDtypeStruct(s, t) for s, t in outs),
            in_specs=specs,
            out_specs=tuple(pl.BlockSpec(memory_space=pltpu.VMEM) for _ in outs),
            scratch_shapes=list(scratch),
            compiler_params=pltpu.CompilerParams(vmem_limit_bytes=56 * 1024 * 1024),
        )(*args)

    return run


def half_start(core, half):
    return pl.multiple_of(core * half, half)


def norm_kernel(at, hidden, cot, scale, shift, gate, own, s1, s2, s3, branch):
    y, core = at[0], at[1]
    values = hidden[...].astype(F32)
    center = values - jnp.mean(values, axis=-1, keepdims=True)
    inverse = lax.rsqrt(jnp.mean(center * center, axis=-1, keepdims=True) + EPSILON)
    normed = (center * inverse * (1.0 + scale[...]) + shift[...]).astype(BF16)
    graded = (cot[...].astype(F32) * gate[...]).astype(BF16)
    branch[...] = graded
    own[...] = jnp.where(y == GRAD_ROLE, graded, normed)
    half = s1.shape[1]
    for j, sent in ((1, s1), (2, s2), (3, s3)):
        wanted = lax.rem(y + j, ROLES) == GRAD_ROLE

        @pl.when(core == 0)
        def _():
            sent[...] = jnp.where(wanted, graded[:, :half], normed[:, :half])

        @pl.when(core == 1)
        def _():
            sent[...] = jnp.where(wanted, graded[:, half:], normed[:, half:])


def project_kernel(at, own, m1, m2, m3, o1, o2, o3, weight, gains, q_out, kv_out, raw_out):
    y, core = at[0], at[1]
    half = m1.shape[1]
    here, there = half_start(core, half), half_start(1 - core, half)
    mine = jnp.concatenate([own[:, pl.ds(here, half)], m1[...], m2[...], m3[...]], axis=0)
    other = jnp.concatenate([own[:, pl.ds(there, half)], o1[...], o2[...], o3[...]], axis=0)
    total = nn(mine, weight[pl.ds(here, half), :]) + nn(other, weight[pl.ds(there, half), :])
    plain = y == GRAD_ROLE
    for at_column, gain, factor, out, column in (
        (0, 0, FACTOR, q_out, 0),
        (1, 1, 1.0, kv_out, 0),
    ):
        raw = total[:, at_column * HEAD_DIM : (at_column + 1) * HEAD_DIM]
        inverse = lax.rsqrt(jnp.mean(raw * raw, axis=-1, keepdims=True) + EPSILON)
        headed = raw * inverse * gains[gain : gain + 1, :] * factor
        out[:, column : column + HEAD_DIM] = jnp.where(plain, raw, headed).astype(BF16)
    kv_out[:, HEAD_DIM:] = total[:, 2 * HEAD_DIM :].astype(BF16)
    raw_out[...] = total[:, : 2 * HEAD_DIM]


def stats_kernel(q0, q1, g0, g1, kv0, kv1, kv2, kv3, stats, mix_own, mix_other, q_all, g_all):
    rows = q0.shape[0]
    q_all[:rows, :] = q0[...]
    q_all[rows:, :] = q1[...]
    g_all[:rows, :] = g0[...]
    g_all[rows:, :] = g1[...]
    pieces = (kv0, kv1, kv2, kv3)
    keys = jnp.concatenate([p[:, :HEAD_DIM] for p in pieces], axis=0)
    values = jnp.concatenate([p[:, HEAD_DIM:] for p in pieces], axis=0)
    values_t = jnp.transpose(values)
    for half, mixed in ((0, mix_own), (1, mix_other)):

        def step(i, carry):
            at = pl.multiple_of(half * rows + i * TILE, TILE)
            local = pl.multiple_of(i * TILE, TILE)
            query = q_all[pl.ds(at, TILE), :]
            grad = g_all[pl.ds(at, TILE), :]
            scores = nt(keys, query)
            top = jnp.max(scores, axis=0, keepdims=True)
            expo = jnp.exp(scores - top)
            total = jnp.sum(expo, axis=0, keepdims=True)
            mix_t = nn(values_t, expo.astype(BF16))
            grad_t = jnp.transpose(grad.astype(F32))
            delta = jnp.sum(mix_t * grad_t, axis=0, keepdims=True)
            stats[0:1, pl.ds(at, TILE)] = top
            stats[1:2, pl.ds(at, TILE)] = total
            stats[2:3, pl.ds(at, TILE)] = delta
            mixed[:, pl.ds(local, TILE)] = mix_t.astype(mixed.dtype)
            return carry

        lax.fori_loop(0, rows // TILE, step, 0)
    stats[3:8, :] = jnp.zeros((5, stats.shape[1]), F32)


def combined(mine, theirs):
    top = jnp.maximum(mine[0:1, :], theirs[0:1, :])
    a, b = jnp.exp(mine[0:1, :] - top), jnp.exp(theirs[0:1, :] - top)
    total = mine[1:2, :] * a + theirs[1:2, :] * b
    delta = (mine[2:3, :] * a + theirs[2:3, :] * b) / total
    return (top, total, delta, a, b)


def grads_kernel(
    q0, q1, g0, g1, kv0, kv1, kv2, kv3, stats, sent, dq0, dq1, dkv0, dkv1, dkv2, dkv3,
    q_all, g_all, level, key_acc, value_acc, query_acc,
):
    rows = q0.shape[0]
    q_all[:rows, :] = q0[...]
    q_all[rows:, :] = q1[...]
    g_all[:rows, :] = g0[...]
    g_all[rows:, :] = g1[...]
    for here, there in ((0, rows), (rows, 0)):
        top, total, delta, _, _ = combined(stats[:, here : here + rows], sent[:, there : there + rows])
        level[0:1, here : here + rows] = top + jnp.log(total)
        level[1:2, here : here + rows] = delta
    pieces = (kv0, kv1, kv2, kv3)
    keys = jnp.concatenate([p[:, :HEAD_DIM] for p in pieces], axis=0)
    values = jnp.concatenate([p[:, HEAD_DIM:] for p in pieces], axis=0)
    keys_t = jnp.transpose(keys)
    key_acc[...] = jnp.zeros(key_acc.shape, F32)
    value_acc[...] = jnp.zeros(value_acc.shape, F32)

    def step(i, carry):
        at = pl.multiple_of(i * TILE, TILE)
        query = q_all[pl.ds(at, TILE), :]
        grad = g_all[pl.ds(at, TILE), :]
        probs = jnp.exp(nt(keys, query) - level[0:1, pl.ds(at, TILE)])
        score_grad = (probs * (nt(values, grad) - level[1:2, pl.ds(at, TILE)])).astype(BF16)
        value_acc[...] += nn(probs.astype(BF16), grad)
        key_acc[...] += nn(score_grad, query)
        query_acc[pl.ds(at, TILE), :] = jnp.transpose(nn(keys_t, score_grad))
        return carry

    lax.fori_loop(0, 2 * rows // TILE, step, 0)
    dq0[...] = query_acc[:rows, :]
    dq1[...] = query_acc[rows:, :].astype(BF16)
    for n, out in enumerate((dkv0, dkv1, dkv2, dkv3)):
        at = slice(n * rows, (n + 1) * rows)
        out[:, :HEAD_DIM] = key_acc[at, :].astype(out.dtype)
        out[:, HEAD_DIM:] = value_acc[at, :].astype(out.dtype)


def mix_kernel(stats, sent, own, other, m0, m1, m2, m3):
    rows = own.shape[1]
    _, total, _, a, b = combined(stats[:, :rows], sent[:, rows:])
    mixed = jnp.transpose((own[...] * a + other[...].astype(F32) * b) / total).astype(BF16)
    block = rows // 4
    for n, out in enumerate((m0, m1, m2, m3)):
        out[...] = mixed[n * block : (n + 1) * block, :]


def head_back(grad, raw, gain, factor):
    inverse = lax.rsqrt(jnp.mean(raw * raw, axis=-1, keepdims=True) + EPSILON)
    unit = raw * inverse
    scaled = grad * gain * factor
    along = jnp.mean(scaled * unit, axis=-1, keepdims=True)
    return (inverse * (scaled - unit * along)).astype(BF16)


def back_kernel(at, dq0, dq1, dkv0, dkv1, dkv2, dkv3, raw, gains, weight, kept, sent):
    y, core = at[0], at[1]
    half = kept.shape[1]
    here, there = half_start(core, half), half_start(1 - core, half)
    query_grad = dq0[...] + dq1[...].astype(F32)
    both = dkv0[...] + dkv1[...].astype(F32) + dkv2[...].astype(F32) + dkv3[...].astype(F32)
    query_raw = head_back(query_grad, raw[:, :HEAD_DIM], gains[0:1, :], FACTOR)
    key_raw = head_back(both[:, :HEAD_DIM], raw[:, HEAD_DIM:], gains[1:2, :], 1.0)
    value_raw = both[:, HEAD_DIM:].astype(BF16)
    grads = jnp.concatenate([query_raw, key_raw, value_raw], axis=1)
    grads = jnp.where(y == GRAD_ROLE, jnp.zeros_like(grads), grads)
    sent[...] = nt(grads, weight[pl.ds(there, half), :]).astype(BF16)
    kept[...] = nt(grads, weight[pl.ds(here, half), :]).astype(BF16)


def pair_kernel(kept, got, p0, p1, p2, p3):
    block = p0.shape[0]
    for n, out in enumerate((p0, p1, p2, p3)):
        at = slice(n * block, (n + 1) * block)
        out[...] = (kept[at, :].astype(F32) + got[at, :].astype(F32)).astype(BF16)


def line_kernel(p0, p1, p2, p3, out):
    total = p0[...].astype(F32) + p1[...].astype(F32) + p2[...].astype(F32) + p3[...].astype(F32)
    out[...] = total.astype(BF16)


def last_kernel(at, hidden, mine, other, scale, out, grad):
    half = mine.shape[1]
    here, there = half_start(at[1], half), half_start(1 - at[1], half)
    grad[:, pl.ds(here, half)] = mine[...].astype(F32)
    grad[:, pl.ds(there, half)] = other[...].astype(F32)
    values = hidden[...].astype(F32)
    center = values - jnp.mean(values, axis=-1, keepdims=True)
    inverse = lax.rsqrt(jnp.mean(center * center, axis=-1, keepdims=True) + EPSILON)
    unit = center * inverse
    scaled = grad[...] * (1.0 + scale[...])
    middle = jnp.mean(scaled, axis=-1, keepdims=True)
    along = jnp.mean(scaled * unit, axis=-1, keepdims=True)
    out[...] = (inverse * (scaled - middle - unit * along)).astype(BF16)


def sum_in_order(pieces, axes, sequence):
    dims = [lax.axis_size(a) for a in axes]
    pieces = pieces.reshape(*dims, *pieces.shape[1:])
    pieces = pieces.transpose(*sequence, *range(len(axes), pieces.ndim))
    pieces = pieces.reshape(-1, *pieces.shape[len(axes) :])
    for k in sequence:
        pieces = lax.psum_scatter(pieces, axes[k], scatter_dimension=0, tiled=True)
    return pieces[0]


def body(
    hidden,
    cotangent,
    mod_scale,
    mod_shift,
    branch_gate,
    query_weight,
    key_weight,
    value_weight,
    output_weight,
    query_gain,
    key_gain,
):
    rows, width = hidden.shape
    half = width // 2
    line = ROLES * rows
    own_rows = query_weight.shape[0]
    columns = 3 * HEAD_DIM
    y = lax.axis_index("y")
    at = jnp.stack([y, lax.axis_index("core")]).astype(jnp.int32)
    scale, shift, gate = mod_scale[None], mod_shift[None], branch_gate[None]
    gains = jnp.stack(
        [lax.dynamic_slice_in_dim(g, y * HEAD_DIM, HEAD_DIM) for g in (query_gain, key_gain)]
    )

    by_role = [
        jnp.concatenate(
            [w[:, h * HEAD_DIM : (h + 1) * HEAD_DIM] for w in (query_weight, key_weight, value_weight)],
            axis=1,
        )
        for h in range(3)
    ] + [output_weight]
    by_role = jnp.stack(by_role)[:, None]
    by_role = jnp.broadcast_to(by_role, (ROLES, 8, own_rows, columns)).reshape(32, own_rows, columns)
    weight = lax.all_to_all(by_role, SEQ, 0, 0, tiled=True).reshape(width, columns)

    own, s1, s2, s3, branch = call(
        norm_kernel,
        [((rows, width), BF16)] + [((rows, half), BF16)] * 3 + [((rows, width), BF16)],
    )(at, hidden, cotangent, scale, shift, gate)
    mine = [shifted(s, "y", j) for j, s in ((1, s1), (2, s2), (3, s3))]
    other = [shifted(m, "core", 1) for m in mine]
    query, kv, raw = call(
        project_kernel,
        [((line, HEAD_DIM), BF16), ((line, 2 * HEAD_DIM), BF16), ((line, 2 * HEAD_DIM), F32)],
    )(at, own, *mine, *other, weight, gains)

    kvs = [kv] + [shifted(kv, "x", j) for j in (1, 2, 3)]
    query_there = shifted(query, "z", 1)
    grad_heads = (query, kv[:, :HEAD_DIM], kv[:, HEAD_DIM:])
    grad = None
    for h in range(3):
        blocks = [(GRAD_ROLE - h + j) % ROLES for j in range(ROLES)]
        ordered = jnp.concatenate([grad_heads[h][i * rows : (i + 1) * rows] for i in blocks], axis=0)
        got = lax.ppermute(ordered, "y", [(GRAD_ROLE, h)])
        grad = got if grad is None else grad + got
    grad_there = shifted(grad, "z", 1)

    both = 2 * line
    stats, mix_own, mix_there = call(
        stats_kernel,
        [((8, both), F32), ((HEAD_DIM, line), F32), ((HEAD_DIM, line), BF16)],
        [pltpu.VMEM((both, HEAD_DIM), BF16), pltpu.VMEM((both, HEAD_DIM), BF16)],
        0,
    )(query, query_there, grad, grad_there, *kvs)
    sent_stats = shifted(stats, "z", 1)
    mix_got = shifted(mix_there, "z", 1)
    dq0, dq1, *dkvs = call(
        grads_kernel,
        [((line, HEAD_DIM), F32), ((line, HEAD_DIM), BF16), ((line, 2 * HEAD_DIM), F32)]
        + [((line, 2 * HEAD_DIM), BF16)] * 3,
        [
            pltpu.VMEM((both, HEAD_DIM), BF16),
            pltpu.VMEM((both, HEAD_DIM), BF16),
            pltpu.VMEM((8, both), F32),
            pltpu.VMEM((4 * line, HEAD_DIM), F32),
            pltpu.VMEM((4 * line, HEAD_DIM), F32),
            pltpu.VMEM((both, HEAD_DIM), F32),
        ],
        0,
    )(query, query_there, grad, grad_there, *kvs, stats, sent_stats)
    dq_got = shifted(dq1, "z", 1)
    dkv_got = [shifted(d, "x", -j) for j, d in zip((1, 2, 3), dkvs[1:])]

    mixes = call(mix_kernel, [((rows, HEAD_DIM), BF16)] * 4, (), 0)(stats, sent_stats, mix_own, mix_got)
    mixes = [mixes[0]] + [shifted(m, "y", -j, range(3)) for j, m in zip((1, 2, 3), mixes[1:])]
    mixes = jnp.concatenate(list(mixes) * 2, axis=1)
    mix = lax.dynamic_slice_in_dim(mixes, lax.rem(ROLES - y, ROLES) * HEAD_DIM, columns, axis=1)
    partial = lax.dot_general(branch, mix, (((0,), (0,)), ((), ())), preferred_element_type=F32)
    partial = partial.astype(BF16).reshape(32, own_rows, columns)
    outproj_grad = sum_in_order(partial, SEQ, (0, 2, 1)).astype(F32)

    kept, sent = call(back_kernel, [((line, half), BF16)] * 2)(
        at, dq0, dq_got, dkvs[0], *dkv_got, raw, gains, weight
    )
    got = shifted(sent, "core", 1)
    parts = call(pair_kernel, [((rows, half), BF16)] * 4, (), 0)(kept, got)
    parts = [parts[0]] + [shifted(p, "y", -j, range(3)) for j, p in zip((1, 2, 3), parts[1:])]
    (chip,) = call(line_kernel, [((rows, half), BF16)], (), 0)(*parts)
    chip_got = shifted(chip, "zlo", 1)
    total = (chip.astype(F32) + chip_got.astype(F32)).astype(BF16)
    total_other = shifted(total, "core", 1)
    (hidden_grad,) = call(
        last_kernel, [((rows, width), BF16)], [pltpu.VMEM((rows, width), F32)]
    )(at, hidden, total, total_other, scale)
    return (hidden_grad, outproj_grad)


def solution(mesh):
    torus = Mesh(mesh.devices.reshape(4, 2, 4, 2, 2), ("y", "z", "x", "zlo", "core"))
    head = ("zlo", "core")
    return jax.shard_map(
        body,
        mesh=torus,
        in_specs=(
            P(SEQ, None),
            P(SEQ, None),
            P(),
            P(),
            P(),
            P(SEQ, head),
            P(SEQ, head),
            P(SEQ, head),
            P(SEQ, head),
            P(head),
            P(head),
        ),
        out_specs=(P(SEQ, None), P(SEQ, head)),
        check_vma=False,
    )
```

```python
import math

import jax
import jax.numpy as jnp
from jax import lax
from jax.experimental import pallas as pl
from jax.experimental.pallas import tpu as pltpu
from jax.sharding import Mesh
from jax.sharding import PartitionSpec as P

HEAD_DIM = 128
SEQ = ("y", "z", "x")
EPSILON = 1e-06
FACTOR = 1.0 / math.sqrt(HEAD_DIM)
ROLES = 4
GRAD_ROLE = 3
TILE = 256
F32 = jnp.float32
BF16 = jnp.bfloat16


def nt(a, b):
    return lax.dot_general(a, b, (((1,), (1,)), ((), ())), preferred_element_type=F32)


def nn(a, b):
    return lax.dot_general(a, b, (((1,), (0,)), ((), ())), preferred_element_type=F32)


def shifted(array, axis, shift, sources=None):
    peers = lax.axis_size(axis)
    sources = range(peers) if sources is None else sources
    return lax.ppermute(array, axis, [(i, (i + shift) % peers) for i in sources])


def exchanged(array, axes):
    return lax.all_to_all(array, axes, 0, 0, tiled=True)


def call(kernel, outs, scratch=(), scalars=1):
    def run(*args):
        specs = [pl.BlockSpec(memory_space=pltpu.SMEM)] * scalars
        specs += [pl.BlockSpec(memory_space=pltpu.VMEM)] * (len(args) - scalars)
        return pl.pallas_call(
            kernel,
            out_shape=tuple(jax.ShapeDtypeStruct(s, t) for s, t in outs),
            in_specs=specs,
            out_specs=tuple(pl.BlockSpec(memory_space=pltpu.VMEM) for _ in outs),
            scratch_shapes=list(scratch),
            compiler_params=pltpu.CompilerParams(vmem_limit_bytes=56 * 1024 * 1024),
        )(*args)

    return run


def half_start(core, half):
    return pl.multiple_of(core * half, half)


def pack_kernel(query, key, value, output, packed):
    for h in range(GRAD_ROLE):
        at = slice(h * HEAD_DIM, (h + 1) * HEAD_DIM)
        for n, source in enumerate((query, key, value)):
            packed[h, :, n * HEAD_DIM : (n + 1) * HEAD_DIM] = source[:, at]
    packed[GRAD_ROLE] = output[...]


def norm_kernel(at, hidden, cot, scale, shift, gate, own, s1, s2, s3, c0, c1, c2, c3):
    y, core = at[0], at[1]
    values = hidden[...].astype(F32)
    center = values - jnp.mean(values, axis=-1, keepdims=True)
    inverse = lax.rsqrt(jnp.mean(center * center, axis=-1, keepdims=True) + EPSILON)
    normed = (center * inverse * (1.0 + scale[...]) + shift[...]).astype(BF16)
    graded = (cot[...].astype(F32) * gate[...]).astype(BF16)
    quarter = c0.shape[1]
    for n in range(ROLES):
        for j, part in enumerate((c0, c1, c2, c3)):

            @pl.when(lax.rem(y + j, ROLES) == n)
            def _():
                part[...] = graded[:, n * quarter : (n + 1) * quarter]

    own[...] = jnp.where(y == GRAD_ROLE, graded, normed)
    half = s1.shape[1]
    for j, sent in ((1, s1), (2, s2), (3, s3)):
        wanted = lax.rem(y + j, ROLES) == GRAD_ROLE

        @pl.when(core == 0)
        def _():
            sent[...] = jnp.where(wanted, graded[:, :half], normed[:, :half])

        @pl.when(core == 1)
        def _():
            sent[...] = jnp.where(wanted, graded[:, half:], normed[:, half:])


def project_kernel(
    at, own, m1, m2, m3, o1, o2, o3, pieces, gains, q_out, kv_out, raw_out, g0, g1, g2, weight
):
    y, core = at[0], at[1]
    groups, _, block, _ = pieces.shape
    for n in range(groups):
        for k in range(ROLES):
            at_row = (k * groups + n) * block
            weight[at_row : at_row + block, :] = pieces[n, k]
    half = m1.shape[1]
    here, there = half_start(core, half), half_start(1 - core, half)
    mine = jnp.concatenate([own[:, pl.ds(here, half)], m1[...], m2[...], m3[...]], axis=0)
    other = jnp.concatenate([own[:, pl.ds(there, half)], o1[...], o2[...], o3[...]], axis=0)
    total = nn(mine, weight[pl.ds(here, half), :]) + nn(other, weight[pl.ds(there, half), :])
    plain = y == GRAD_ROLE
    for at_column, gain, factor, out, column in (
        (0, 0, FACTOR, q_out, 0),
        (1, 1, 1.0, kv_out, 0),
    ):
        raw = total[:, at_column * HEAD_DIM : (at_column + 1) * HEAD_DIM]
        inverse = lax.rsqrt(jnp.mean(raw * raw, axis=-1, keepdims=True) + EPSILON)
        headed = raw * inverse * gains[gain : gain + 1, :] * factor
        out[:, column : column + HEAD_DIM] = jnp.where(plain, raw, headed).astype(BF16)
    kv_out[:, HEAD_DIM:] = total[:, 2 * HEAD_DIM :].astype(BF16)
    raw_out[...] = total[:, : 2 * HEAD_DIM]
    rows = own.shape[0]
    for h, out in enumerate((g0, g1, g2)):
        for j in range(ROLES):
            i = (GRAD_ROLE - h + j) % ROLES
            piece = total[i * rows : (i + 1) * rows, h * HEAD_DIM : (h + 1) * HEAD_DIM]
            out[j * rows : (j + 1) * rows, :] = piece.astype(BF16)


def stats_kernel(q0, q1, g0, g1, kv0, kv1, kv2, kv3, stats, mix_own, mix_other, q_all, g_all):
    rows = q0.shape[0]
    q_all[:rows, :] = q0[...]
    q_all[rows:, :] = q1[...]
    g_all[:rows, :] = g0[...]
    g_all[rows:, :] = g1[...]
    pieces = (kv0, kv1, kv2, kv3)
    keys = jnp.concatenate([p[:, :HEAD_DIM] for p in pieces], axis=0)
    values = jnp.concatenate([p[:, HEAD_DIM:] for p in pieces], axis=0)
    values_t = jnp.transpose(values)
    for half, mixed in ((0, mix_own), (1, mix_other)):

        def step(i, carry):
            at = pl.multiple_of(half * rows + i * TILE, TILE)
            local = pl.multiple_of(i * TILE, TILE)
            query = q_all[pl.ds(at, TILE), :]
            grad = g_all[pl.ds(at, TILE), :]
            scores = nt(keys, query)
            top = jnp.max(scores, axis=0, keepdims=True)
            expo = jnp.exp(scores - top)
            total = jnp.sum(expo, axis=0, keepdims=True)
            mix_t = nn(values_t, expo.astype(BF16))
            grad_t = jnp.transpose(grad.astype(F32))
            delta = jnp.sum(mix_t * grad_t, axis=0, keepdims=True)
            stats[0:1, pl.ds(at, TILE)] = top
            stats[1:2, pl.ds(at, TILE)] = total
            stats[2:3, pl.ds(at, TILE)] = delta
            mixed[:, pl.ds(local, TILE)] = mix_t.astype(mixed.dtype)
            return carry

        lax.fori_loop(0, rows // TILE, step, 0)
    stats[3:8, :] = jnp.zeros((5, stats.shape[1]), F32)


def combined(mine, theirs):
    top = jnp.maximum(mine[0:1, :], theirs[0:1, :])
    a, b = jnp.exp(mine[0:1, :] - top), jnp.exp(theirs[0:1, :] - top)
    total = mine[1:2, :] * a + theirs[1:2, :] * b
    delta = (mine[2:3, :] * a + theirs[2:3, :] * b) / total
    return (top, total, delta, a, b)


def grads_kernel(
    q0, q1, g0, g1, kv0, kv1, kv2, kv3, stats, sent, dq0, dq1, dkv0, dkv1, dkv2, dkv3,
    q_all, g_all, level, key_acc, value_acc, query_acc,
):
    rows = q0.shape[0]
    q_all[:rows, :] = q0[...]
    q_all[rows:, :] = q1[...]
    g_all[:rows, :] = g0[...]
    g_all[rows:, :] = g1[...]
    for here, there in ((0, rows), (rows, 0)):
        top, total, delta, _, _ = combined(stats[:, here : here + rows], sent[:, there : there + rows])
        level[0:1, here : here + rows] = top + jnp.log(total)
        level[1:2, here : here + rows] = delta
    pieces = (kv0, kv1, kv2, kv3)
    keys = jnp.concatenate([p[:, :HEAD_DIM] for p in pieces], axis=0)
    values = jnp.concatenate([p[:, HEAD_DIM:] for p in pieces], axis=0)
    keys_t = jnp.transpose(keys)
    key_acc[...] = jnp.zeros(key_acc.shape, F32)
    value_acc[...] = jnp.zeros(value_acc.shape, F32)

    def step(i, carry):
        at = pl.multiple_of(i * TILE, TILE)
        query = q_all[pl.ds(at, TILE), :]
        grad = g_all[pl.ds(at, TILE), :]
        probs = jnp.exp(nt(keys, query) - level[0:1, pl.ds(at, TILE)])
        score_grad = (probs * (nt(values, grad) - level[1:2, pl.ds(at, TILE)])).astype(BF16)
        value_acc[...] += nn(probs.astype(BF16), grad)
        key_acc[...] += nn(score_grad, query)
        query_acc[pl.ds(at, TILE), :] = jnp.transpose(nn(keys_t, score_grad))
        return carry

    lax.fori_loop(0, 2 * rows // TILE, step, 0)
    dq0[...] = query_acc[:rows, :]
    dq1[...] = query_acc[rows:, :].astype(BF16)
    for n, out in enumerate((dkv0, dkv1, dkv2, dkv3)):
        at = slice(n * rows, (n + 1) * rows)
        out[:, :HEAD_DIM] = key_acc[at, :].astype(out.dtype)
        out[:, HEAD_DIM:] = value_acc[at, :].astype(out.dtype)


def mix_kernel(stats, sent, own, other, m0, m1, m2, m3):
    rows = own.shape[1]
    _, total, _, a, b = combined(stats[:, :rows], sent[:, rows:])
    mixed = jnp.transpose((own[...] * a + other[...].astype(F32) * b) / total).astype(BF16)
    block = rows // ROLES
    for shift, out in enumerate((m0, m1, m2, m3)):
        for j in range(ROLES):
            i = (j - shift) % ROLES
            out[j * block : (j + 1) * block, :] = mixed[i * block : (i + 1) * block, :]


def outproj_kernel(at, m0, m1, m2, m3, c0, c1, c2, c3, out, mixes):
    y = at[0]
    for shift, part in enumerate((m0, m1, m2, m3)):
        head = lax.rem(y + ROLES - shift, ROLES)
        mixes[:, pl.ds(pl.multiple_of(head * HEAD_DIM, HEAD_DIM), HEAD_DIM)] = part[...]
    cot = jnp.concatenate([c0[...], c1[...], c2[...], c3[...]], axis=0)
    total = nn(jnp.transpose(cot), mixes[:, : GRAD_ROLE * HEAD_DIM]).astype(BF16)
    block = out.shape[1]
    for n in range(out.shape[0]):
        out[n] = total[n * block : (n + 1) * block, :]


def sum_kernel(parts, out):
    total = parts[0].astype(F32)
    for n in range(1, parts.shape[0]):
        total = total + parts[n].astype(F32)
    out[...] = total


def head_back(grad, raw, gain, factor):
    inverse = lax.rsqrt(jnp.mean(raw * raw, axis=-1, keepdims=True) + EPSILON)
    unit = raw * inverse
    scaled = grad * gain * factor
    along = jnp.mean(scaled * unit, axis=-1, keepdims=True)
    return (inverse * (scaled - unit * along)).astype(BF16)


def back_kernel(at, dq0, dq1, dkv0, dkv1, dkv2, dkv3, raw, gains, weight, kept, sent):
    y, core = at[0], at[1]
    half = kept.shape[1]
    here, there = half_start(core, half), half_start(1 - core, half)
    query_grad = dq0[...] + dq1[...].astype(F32)
    both = dkv0[...] + dkv1[...].astype(F32) + dkv2[...].astype(F32) + dkv3[...].astype(F32)
    query_raw = head_back(query_grad, raw[:, :HEAD_DIM], gains[0:1, :], FACTOR)
    key_raw = head_back(both[:, :HEAD_DIM], raw[:, HEAD_DIM:], gains[1:2, :], 1.0)
    value_raw = both[:, HEAD_DIM:].astype(BF16)
    grads = jnp.concatenate([query_raw, key_raw, value_raw], axis=1)
    grads = jnp.where(y == GRAD_ROLE, jnp.zeros_like(grads), grads)
    sent[...] = nt(grads, weight[pl.ds(there, half), :]).astype(BF16)
    kept[...] = nt(grads, weight[pl.ds(here, half), :]).astype(BF16)


def pair_kernel(kept, got, p0, p1, p2, p3):
    block = p0.shape[0]
    for n, out in enumerate((p0, p1, p2, p3)):
        at = slice(n * block, (n + 1) * block)
        out[...] = (kept[at, :].astype(F32) + got[at, :].astype(F32)).astype(BF16)


def line_kernel(p0, p1, p2, p3, out):
    total = p0[...].astype(F32) + p1[...].astype(F32) + p2[...].astype(F32) + p3[...].astype(F32)
    out[...] = total.astype(BF16)


def last_kernel(at, hidden, mine, other, scale, out, grad):
    half = mine.shape[1]
    here, there = half_start(at[1], half), half_start(1 - at[1], half)
    grad[:, pl.ds(here, half)] = mine[...].astype(F32)
    grad[:, pl.ds(there, half)] = other[...].astype(F32)
    values = hidden[...].astype(F32)
    center = values - jnp.mean(values, axis=-1, keepdims=True)
    inverse = lax.rsqrt(jnp.mean(center * center, axis=-1, keepdims=True) + EPSILON)
    unit = center * inverse
    scaled = grad[...] * (1.0 + scale[...])
    middle = jnp.mean(scaled, axis=-1, keepdims=True)
    along = jnp.mean(scaled * unit, axis=-1, keepdims=True)
    out[...] = (inverse * (scaled - middle - unit * along)).astype(BF16)


def body(
    hidden,
    cotangent,
    mod_scale,
    mod_shift,
    branch_gate,
    query_weight,
    key_weight,
    value_weight,
    output_weight,
    query_gain,
    key_gain,
):
    rows, width = hidden.shape
    half = width // 2
    line = ROLES * rows
    own_rows = query_weight.shape[0]
    columns = 3 * HEAD_DIM
    y = lax.axis_index("y")
    at = jnp.stack([y, lax.axis_index("core")]).astype(jnp.int32)
    scale, shift, gate = mod_scale[None], mod_shift[None], branch_gate[None]
    gains = jnp.stack(
        [lax.dynamic_slice_in_dim(g, y * HEAD_DIM, HEAD_DIM) for g in (query_gain, key_gain)]
    )

    (packed,) = call(pack_kernel, [((ROLES, own_rows, columns), BF16)], (), 0)(
        query_weight, key_weight, value_weight, output_weight
    )
    packed = exchanged(packed, "y")
    packed = jnp.broadcast_to(packed[None], (8, *packed.shape))
    pieces = exchanged(packed, ("z", "x"))

    own, s1, s2, s3, *cots = call(
        norm_kernel,
        [((rows, width), BF16)] + [((rows, half), BF16)] * 3 + [((rows, width // ROLES), BF16)] * 4,
    )(at, hidden, cotangent, scale, shift, gate)
    mine = [shifted(s, "y", j) for j, s in ((1, s1), (2, s2), (3, s3))]
    other = [shifted(m, "core", 1) for m in mine]
    query, kv, raw, *grad_sent, weight = call(
        project_kernel,
        [((line, HEAD_DIM), BF16), ((line, 2 * HEAD_DIM), BF16), ((line, 2 * HEAD_DIM), F32)]
        + [((line, HEAD_DIM), BF16)] * 3
        + [((width, columns), BF16)],
    )(at, own, *mine, *other, pieces, gains)

    kvs = [kv] + [shifted(kv, "x", j) for j in (1, 2, 3)]
    query_there = shifted(query, "z", 1)
    got = [shifted(g, "y", h - GRAD_ROLE, [GRAD_ROLE]) for h, g in enumerate(grad_sent)]
    grad = got[0] + got[1] + got[2]
    grad_there = shifted(grad, "z", 1)

    both = 2 * line
    stats, mix_own, mix_there = call(
        stats_kernel,
        [((8, both), F32), ((HEAD_DIM, line), F32), ((HEAD_DIM, line), BF16)],
        [pltpu.VMEM((both, HEAD_DIM), BF16), pltpu.VMEM((both, HEAD_DIM), BF16)],
        0,
    )(query, query_there, grad, grad_there, *kvs)
    sent_stats = shifted(stats, "z", 1)
    mix_got = shifted(mix_there, "z", 1)
    dq0, dq1, *dkvs = call(
        grads_kernel,
        [((line, HEAD_DIM), F32), ((line, HEAD_DIM), BF16), ((line, 2 * HEAD_DIM), F32)]
        + [((line, 2 * HEAD_DIM), BF16)] * 3,
        [
            pltpu.VMEM((both, HEAD_DIM), BF16),
            pltpu.VMEM((both, HEAD_DIM), BF16),
            pltpu.VMEM((8, both), F32),
            pltpu.VMEM((4 * line, HEAD_DIM), F32),
            pltpu.VMEM((4 * line, HEAD_DIM), F32),
            pltpu.VMEM((both, HEAD_DIM), F32),
        ],
        0,
    )(query, query_there, grad, grad_there, *kvs, stats, sent_stats)
    dq_got = shifted(dq1, "z", 1)
    dkv_got = [shifted(d, "x", -j) for j, d in zip((1, 2, 3), dkvs[1:])]

    cots = [cots[0]] + [shifted(c, "y", j) for j, c in zip((1, 2, 3), cots[1:])]
    mixes = call(mix_kernel, [((line, HEAD_DIM), BF16)] * 4, (), 0)(stats, sent_stats, mix_own, mix_got)
    mixes = [mixes[0]] + [shifted(m, "y", j, range(3)) for j, m in zip((1, 2, 3), mixes[1:])]
    (partial,) = call(
        outproj_kernel, [((8, own_rows, columns), BF16)], [pltpu.VMEM((line, ROLES * HEAD_DIM), BF16)]
    )(at, *mixes, *cots)
    partial = exchanged(partial, ("z", "x"))
    (outproj_grad,) = call(sum_kernel, [((own_rows, columns), F32)], (), 0)(partial)

    kept, sent = call(back_kernel, [((line, half), BF16)] * 2)(
        at, dq0, dq_got, dkvs[0], *dkv_got, raw, gains, weight
    )
    got = shifted(sent, "core", 1)
    parts = call(pair_kernel, [((rows, half), BF16)] * 4, (), 0)(kept, got)
    parts = [parts[0]] + [shifted(p, "y", -j, range(3)) for j, p in zip((1, 2, 3), parts[1:])]
    (chip,) = call(line_kernel, [((rows, half), BF16)], (), 0)(*parts)
    chip_got = shifted(chip, "zlo", 1)
    total = (chip.astype(F32) + chip_got.astype(F32)).astype(BF16)
    total_other = shifted(total, "core", 1)
    (hidden_grad,) = call(
        last_kernel, [((rows, width), BF16)], [pltpu.VMEM((rows, width), F32)]
    )(at, hidden, total, total_other, scale)
    return (hidden_grad, outproj_grad)


def solution(mesh):
    torus = Mesh(mesh.devices.reshape(4, 2, 4, 2, 2), ("y", "z", "x", "zlo", "core"))
    head = ("zlo", "core")
    return jax.shard_map(
        body,
        mesh=torus,
        in_specs=(
            P(SEQ, None),
            P(SEQ, None),
            P(),
            P(),
            P(),
            P(SEQ, head),
            P(SEQ, head),
            P(SEQ, head),
            P(SEQ, head),
            P(head),
            P(head),
        ),
        out_specs=(P(SEQ, None), P(SEQ, head)),
        check_vma=False,
    )
```

```python
import math

import jax
import jax.numpy as jnp
from jax import lax
from jax.experimental import pallas as pl
from jax.experimental.pallas import tpu as pltpu
from jax.sharding import Mesh
from jax.sharding import PartitionSpec as P

HEAD_DIM = 128
SEQ = ("y", "z", "x")
EPSILON = 1e-06
FACTOR = 1.0 / math.sqrt(HEAD_DIM)
ROLES = 4
GRAD_ROLE = 3
TILE = 256
UNROLL = 2
F32 = jnp.float32
BF16 = jnp.bfloat16


PLANE_ORDER = ((0, 1), (1, 0), (0, 3), (1, 1), (1, 3), (0, 2), (1, 2))


def nt(a, b):
    return lax.dot_general(a, b, (((1,), (1,)), ((), ())), preferred_element_type=F32)


def nn(a, b):
    return lax.dot_general(a, b, (((1,), (0,)), ((), ())), preferred_element_type=F32)


def shifted(array, axis, shift, sources=None):
    peers = lax.axis_size(axis)
    sources = range(peers) if sources is None else sources
    return lax.ppermute(array, axis, [(i, (i + shift) % peers) for i in sources])


def exchanged(array, axes):
    return lax.all_to_all(array, axes, 0, 0, tiled=True)


def call(kernel, outs, scratch=(), scalars=1):
    def run(*args):
        specs = [pl.BlockSpec(memory_space=pltpu.SMEM)] * scalars
        specs += [pl.BlockSpec(memory_space=pltpu.VMEM)] * (len(args) - scalars)
        return pl.pallas_call(
            kernel,
            out_shape=tuple(jax.ShapeDtypeStruct(s, t) for s, t in outs),
            in_specs=specs,
            out_specs=tuple(pl.BlockSpec(memory_space=pltpu.VMEM) for _ in outs),
            scratch_shapes=list(scratch),
            compiler_params=pltpu.CompilerParams(vmem_limit_bytes=56 * 1024 * 1024),
        )(*args)

    return run


def half_start(core, half):
    return pl.multiple_of(core * half, half)


def pack_kernel(at, query, key, value, output, own, s1, s2, s3):
    for j, out in enumerate((own, s1, s2, s3)):
        role = lax.rem(at[0] + j, ROLES)
        for h in range(GRAD_ROLE):

            @pl.when(role == h)
            def _():
                for n, source in enumerate((query, key, value)):
                    here = slice(h * HEAD_DIM, (h + 1) * HEAD_DIM)
                    out[:, n * HEAD_DIM : (n + 1) * HEAD_DIM] = source[:, here]

        @pl.when(role == GRAD_ROLE)
        def _():
            out[...] = output[...]


def norm_kernel(at, hidden, cot, scale, shift, gate, own, s1, s2, s3, branch, branch_half):
    y, core = at[0], at[1]
    values = hidden[...].astype(F32)
    center = values - jnp.mean(values, axis=-1, keepdims=True)
    inverse = lax.rsqrt(jnp.mean(center * center, axis=-1, keepdims=True) + EPSILON)
    normed = (center * inverse * (1.0 + scale[...]) + shift[...]).astype(BF16)
    graded = (cot[...].astype(F32) * gate[...]).astype(BF16)
    branch[...] = graded
    own[...] = jnp.where(y == GRAD_ROLE, graded, normed)
    half = s1.shape[1]

    @pl.when(core == 0)
    def _():
        branch_half[...] = graded[:, :half]

    @pl.when(core == 1)
    def _():
        branch_half[...] = graded[:, half:]

    for j, sent in ((1, s1), (2, s2), (3, s3)):
        wanted = lax.rem(y + j, ROLES) == GRAD_ROLE

        @pl.when(core == 0)
        def _():
            sent[...] = jnp.where(wanted, graded[:, :half], normed[:, :half])

        @pl.when(core == 1)
        def _():
            sent[...] = jnp.where(wanted, graded[:, half:], normed[:, half:])


def project_kernel(
    at, own, m1, m2, m3, o1, o2, o3, w0, w1, w2, w3, w4, w5, w6, w7, gains,
    q_out, kv_out, raw_out, g0, g1, g2, w_here, w_there,
):
    y, core, plane = at[0], at[1], at[2]
    pieces = (w0, w1, w2, w3, w4, w5, w6, w7)
    block = w0.shape[1]
    for (dz, dx), piece in zip(((0, 0), *PLANE_ORDER), pieces):
        source = 4 * lax.rem(plane // 4 + dz, 2) + lax.rem(plane + 4 - dx, 4)
        for t in range(2):
            at_row = pl.multiple_of((t * len(pieces) + source) * block, block)
            w_here[pl.ds(at_row, block), :] = piece[lax.rem(y + ROLES - (2 * core + t), ROLES)]
            w_there[pl.ds(at_row, block), :] = piece[lax.rem(y + ROLES - (2 - 2 * core + t), ROLES)]
    half = m1.shape[1]
    here, there = half_start(core, half), half_start(1 - core, half)
    mine = jnp.concatenate([own[:, pl.ds(here, half)], m1[...], m2[...], m3[...]], axis=0)
    other = jnp.concatenate([own[:, pl.ds(there, half)], o1[...], o2[...], o3[...]], axis=0)
    total = nn(mine, w_here[...]) + nn(other, w_there[...])
    plain = y == GRAD_ROLE
    for at_column, gain, factor, out, column in (
        (0, 0, FACTOR, q_out, 0),
        (1, 1, 1.0, kv_out, 0),
    ):
        raw = total[:, at_column * HEAD_DIM : (at_column + 1) * HEAD_DIM]
        inverse = lax.rsqrt(jnp.mean(raw * raw, axis=-1, keepdims=True) + EPSILON)
        headed = raw * inverse * gains[gain : gain + 1, :] * factor
        out[:, column : column + HEAD_DIM] = jnp.where(plain, raw, headed).astype(BF16)
    kv_out[:, HEAD_DIM:] = total[:, 2 * HEAD_DIM :].astype(BF16)
    raw_out[...] = total[:, : 2 * HEAD_DIM]
    rows = own.shape[0]
    for h, out in enumerate((g0, g1, g2)):
        for j in range(ROLES):
            i = (GRAD_ROLE - h + j) % ROLES
            piece = total[i * rows : (i + 1) * rows, h * HEAD_DIM : (h + 1) * HEAD_DIM]
            out[j * rows : (j + 1) * rows, :] = piece.astype(BF16)


def stats_kernel(q0, q1, g0, g1, kv0, kv1, kv2, kv3, stats, mix_own, mix_other, q_all, g_all):
    rows = q0.shape[0]
    q_all[:rows, :] = q0[...]
    q_all[rows:, :] = q1[...]
    g_all[:rows, :] = g0[...]
    g_all[rows:, :] = g1[...]
    pieces = (kv0, kv1, kv2, kv3)
    keys = jnp.concatenate([p[:, :HEAD_DIM] for p in pieces], axis=0)
    values = jnp.concatenate([p[:, HEAD_DIM:] for p in pieces], axis=0)
    values_t = jnp.transpose(values)
    for half, mixed in ((0, mix_own), (1, mix_other)):

        def step(i, carry):
            at = pl.multiple_of(half * rows + i * TILE, TILE)
            local = pl.multiple_of(i * TILE, TILE)
            query = q_all[pl.ds(at, TILE), :]
            grad = g_all[pl.ds(at, TILE), :]
            scores = nt(keys, query)
            top = jnp.max(scores, axis=0, keepdims=True)
            expo = jnp.exp(scores - top)
            total = jnp.sum(expo, axis=0, keepdims=True)
            mix_t = nn(values_t, expo.astype(BF16))
            grad_t = jnp.transpose(grad.astype(F32))
            delta = jnp.sum(mix_t * grad_t, axis=0, keepdims=True)
            stats[0:1, pl.ds(at, TILE)] = top
            stats[1:2, pl.ds(at, TILE)] = total
            stats[2:3, pl.ds(at, TILE)] = delta
            mixed[:, pl.ds(local, TILE)] = mix_t.astype(mixed.dtype)
            return carry

        lax.fori_loop(0, rows // TILE, step, 0, unroll=True)
    stats[3:8, :] = jnp.zeros((5, stats.shape[1]), F32)


def combined(mine, theirs):
    top = jnp.maximum(mine[0:1, :], theirs[0:1, :])
    a, b = jnp.exp(mine[0:1, :] - top), jnp.exp(theirs[0:1, :] - top)
    total = mine[1:2, :] * a + theirs[1:2, :] * b
    delta = (mine[2:3, :] * a + theirs[2:3, :] * b) / total
    return (top, total, delta, a, b)


def grads_kernel(
    q0, q1, g0, g1, kv0, kv1, kv2, kv3, stats, sent, dq0, dq1, dkv0, dkv1, dkv2, dkv3,
    q_all, g_all, level, key_acc, value_acc, query_acc,
):
    rows = q0.shape[0]
    q_all[:rows, :] = q0[...]
    q_all[rows:, :] = q1[...]
    g_all[:rows, :] = g0[...]
    g_all[rows:, :] = g1[...]
    for here, there in ((0, rows), (rows, 0)):
        top, total, delta, _, _ = combined(stats[:, here : here + rows], sent[:, there : there + rows])
        level[0:1, here : here + rows] = top + jnp.log(total)
        level[1:2, here : here + rows] = delta
    pieces = (kv0, kv1, kv2, kv3)
    keys = jnp.concatenate([p[:, :HEAD_DIM] for p in pieces], axis=0)
    values = jnp.concatenate([p[:, HEAD_DIM:] for p in pieces], axis=0)
    keys_t = jnp.transpose(keys)
    key_acc[...] = jnp.zeros(key_acc.shape, F32)
    value_acc[...] = jnp.zeros(value_acc.shape, F32)

    def step(i, carry):
        at = pl.multiple_of(i * TILE, TILE)
        query = q_all[pl.ds(at, TILE), :]
        grad = g_all[pl.ds(at, TILE), :]
        probs = jnp.exp(nt(keys, query) - level[0:1, pl.ds(at, TILE)])
        score_grad = (probs * (nt(values, grad) - level[1:2, pl.ds(at, TILE)])).astype(BF16)
        value_acc[...] += nn(probs.astype(BF16), grad)
        key_acc[...] += nn(score_grad, query)
        query_acc[pl.ds(at, TILE), :] = jnp.transpose(nn(keys_t, score_grad))
        return carry

    lax.fori_loop(0, 2 * rows // TILE, step, 0, unroll=UNROLL)
    dq0[...] = query_acc[:rows, :]
    dq1[...] = query_acc[rows:, :].astype(BF16)
    for n, out in enumerate((dkv0, dkv1, dkv2, dkv3)):
        at = slice(n * rows, (n + 1) * rows)
        out[:, :HEAD_DIM] = key_acc[at, :].astype(out.dtype)
        out[:, HEAD_DIM:] = value_acc[at, :].astype(out.dtype)


def outproj_kernel(at, stats, sent, own, other, branch, c1, c2, c3, d1, d2, d3, out):
    core = at[1]
    rows, half = own.shape[1], c1.shape[1]
    _, total, _, a, b = combined(stats[:, :rows], sent[:, rows:])
    mix_t = ((own[...] * a + other[...].astype(F32) * b) / total).astype(BF16)
    groups, _, block, _ = out.shape
    for side, parts in ((core, (c1, c2, c3)), (1 - core, (d1, d2, d3))):
        first = branch[:, pl.ds(half_start(side, half), half)]
        cot = jnp.concatenate([first] + [p[...] for p in parts], axis=0)
        partial = jnp.transpose(nn(mix_t, cot)).astype(BF16)
        for n in range(groups):
            for t in range(2):
                at_row = (t * groups + n) * block
                out[n, 2 * side + t] = partial[at_row : at_row + block, :]


def sum_kernel(at, parts, own, s1, s2, s3):
    for j, out in enumerate((own, s1, s2, s3)):
        block = lax.rem(at[0] + ROLES - j, ROLES)
        total = parts[0, block].astype(F32)
        for n in range(1, parts.shape[0]):
            total = total + parts[n, block].astype(F32)
        out[...] = total


def head_back(grad, raw, gain, factor):
    inverse = lax.rsqrt(jnp.mean(raw * raw, axis=-1, keepdims=True) + EPSILON)
    unit = raw * inverse
    scaled = grad * gain * factor
    along = jnp.mean(scaled * unit, axis=-1, keepdims=True)
    return (inverse * (scaled - unit * along)).astype(BF16)


def back_kernel(at, dq0, dq1, dkv0, dkv1, dkv2, dkv3, raw, gains, grads):
    query_grad = dq0[...] + dq1[...].astype(F32)
    both = dkv0[...] + dkv1[...].astype(F32) + dkv2[...].astype(F32) + dkv3[...].astype(F32)
    query_raw = head_back(query_grad, raw[:, :HEAD_DIM], gains[0:1, :], FACTOR)
    key_raw = head_back(both[:, :HEAD_DIM], raw[:, HEAD_DIM:], gains[1:2, :], 1.0)
    value_raw = both[:, HEAD_DIM:].astype(BF16)
    joined = jnp.concatenate([query_raw, key_raw, value_raw], axis=1)
    grads[...] = jnp.where(at[0] == GRAD_ROLE, jnp.zeros_like(joined), joined)


def spread_kernel(mine, other, w_mine, w_other, p0, p1, p2, p3):
    block = p0.shape[0]
    total = nt(mine[...], w_mine[...]) + nt(other[...], w_other[...])
    for n, out in enumerate((p0, p1, p2, p3)):
        out[...] = total[n * block : (n + 1) * block, :].astype(BF16)


def line_kernel(p0, p1, p2, p3, out):
    total = p0[...].astype(F32) + p1[...].astype(F32) + p2[...].astype(F32) + p3[...].astype(F32)
    out[...] = total.astype(BF16)


def last_kernel(at, hidden, a0, a1, b0, b1, scale, o0, o1, o2, o3, out, outproj, grad):
    half = a0.shape[1]
    for j, part in enumerate((o0, o1, o2, o3)):
        head = lax.rem(at[0] + j, ROLES)

        @pl.when(head < GRAD_ROLE)
        def _():
            outproj[:, pl.ds(pl.multiple_of(head * HEAD_DIM, HEAD_DIM), HEAD_DIM)] = part[...]

    here, there = half_start(at[1], half), half_start(1 - at[1], half)
    grad[:, pl.ds(here, half)] = a0[...].astype(F32) + a1[...].astype(F32)
    grad[:, pl.ds(there, half)] = b0[...].astype(F32) + b1[...].astype(F32)
    values = hidden[...].astype(F32)
    center = values - jnp.mean(values, axis=-1, keepdims=True)
    inverse = lax.rsqrt(jnp.mean(center * center, axis=-1, keepdims=True) + EPSILON)
    unit = center * inverse
    scaled = grad[...] * (1.0 + scale[...])
    middle = jnp.mean(scaled, axis=-1, keepdims=True)
    along = jnp.mean(scaled * unit, axis=-1, keepdims=True)
    out[...] = (inverse * (scaled - middle - unit * along)).astype(BF16)


def body(
    hidden,
    cotangent,
    mod_scale,
    mod_shift,
    branch_gate,
    query_weight,
    key_weight,
    value_weight,
    output_weight,
    query_gain,
    key_gain,
):
    rows, width = hidden.shape
    half = width // 2
    line = ROLES * rows
    own_rows = query_weight.shape[0]
    columns = 3 * HEAD_DIM
    y = lax.axis_index("y")
    at = jnp.stack([y, lax.axis_index("core"), lax.axis_index(("z", "x"))]).astype(jnp.int32)
    scale, shift, gate = mod_scale[None], mod_shift[None], branch_gate[None]
    gains = jnp.stack(
        [lax.dynamic_slice_in_dim(g, y * HEAD_DIM, HEAD_DIM) for g in (query_gain, key_gain)]
    )

    packed = call(pack_kernel, [((own_rows, columns), BF16)] * ROLES)(
        at, query_weight, key_weight, value_weight, output_weight
    )
    packed = [packed[0]] + [shifted(p, "y", j) for j, p in zip((1, 2, 3), packed[1:])]
    packed = jnp.stack(packed)
    pieces = [packed]
    for dz, dx in PLANE_ORDER:
        moves = [(4 * z + x, 4 * ((z + dz) % 2) + (x + dx) % 4) for z in range(2) for x in range(4)]
        pieces.append(lax.ppermute(packed, ("z", "x"), moves))

    own, s1, s2, s3, branch, branch_half = call(
        norm_kernel,
        [((rows, width), BF16)] + [((rows, half), BF16)] * 3 + [((rows, width), BF16), ((rows, half), BF16)],
    )(at, hidden, cotangent, scale, shift, gate)
    mine = [shifted(s, "y", j) for j, s in ((1, s1), (2, s2), (3, s3))]
    other = [shifted(m, "core", 1) for m in mine]
    query, kv, raw, *grad_sent, w_here, w_there = call(
        project_kernel,
        [((line, HEAD_DIM), BF16), ((line, 2 * HEAD_DIM), BF16), ((line, 2 * HEAD_DIM), F32)]
        + [((line, HEAD_DIM), BF16)] * 3
        + [((half, columns), BF16)] * 2,
    )(at, own, *mine, *other, *pieces, gains)
    w_other = shifted(w_there, "core", 1)

    kvs = [kv] + [shifted(kv, "x", j) for j in (1, 2, 3)]
    query_there = shifted(query, "z", 1)
    got = [shifted(g, "y", h - GRAD_ROLE, [GRAD_ROLE]) for h, g in enumerate(grad_sent)]
    grad = got[0] + got[1] + got[2]
    grad_there = shifted(grad, "z", 1)

    both = 2 * line
    stats, mix_own, mix_there = call(
        stats_kernel,
        [((8, both), F32), ((HEAD_DIM, line), F32), ((HEAD_DIM, line), BF16)],
        [pltpu.VMEM((both, HEAD_DIM), BF16), pltpu.VMEM((both, HEAD_DIM), BF16)],
        0,
    )(query, query_there, grad, grad_there, *kvs)
    sent_stats = shifted(stats, "z", 1)
    mix_got = shifted(mix_there, "z", 1)
    dq0, dq1, *dkvs = call(
        grads_kernel,
        [((line, HEAD_DIM), F32), ((line, HEAD_DIM), BF16), ((line, 2 * HEAD_DIM), F32)]
        + [((line, 2 * HEAD_DIM), BF16)] * 3,
        [
            pltpu.VMEM((both, HEAD_DIM), BF16),
            pltpu.VMEM((both, HEAD_DIM), BF16),
            pltpu.VMEM((8, both), F32),
            pltpu.VMEM((4 * line, HEAD_DIM), F32),
            pltpu.VMEM((4 * line, HEAD_DIM), F32),
            pltpu.VMEM((both, HEAD_DIM), F32),
        ],
        0,
    )(query, query_there, grad, grad_there, *kvs, stats, sent_stats)
    dq_got = shifted(dq1, "z", 1)
    dkv_got = [shifted(d, "x", -j) for j, d in zip((1, 2, 3), dkvs[1:])]

    cots = [shifted(branch_half, "y", j) for j in (1, 2, 3)]
    cots_other = [shifted(c, "core", 1) for c in cots]
    (partial,) = call(outproj_kernel, [((8, ROLES, own_rows, HEAD_DIM), BF16)])(
        at, stats, sent_stats, mix_own, mix_got, branch, *cots, *cots_other
    )
    partial = exchanged(partial, ("z", "x"))
    summed = call(sum_kernel, [((own_rows, HEAD_DIM), F32)] * ROLES)(at, partial)
    summed = [summed[0]] + [shifted(p, "y", -j, range(3)) for j, p in zip((1, 2, 3), summed[1:])]

    (raw_grads,) = call(back_kernel, [((line, columns), BF16)])(
        at, dq0, dq_got, dkvs[0], *dkv_got, raw, gains
    )
    raw_other = shifted(raw_grads, "core", 1)
    parts = call(spread_kernel, [((rows, half), BF16)] * 4, (), 0)(raw_grads, raw_other, w_here, w_other)
    parts = [parts[0]] + [shifted(p, "y", -j, range(3)) for j, p in zip((1, 2, 3), parts[1:])]
    (chip,) = call(line_kernel, [((rows, half), BF16)], (), 0)(*parts)
    chip_got = shifted(chip, "zlo", 1)
    chip_other = shifted(chip, "core", 1)
    got_other = shifted(chip_got, "core", 1)
    hidden_grad, outproj_grad = call(
        last_kernel,
        [((rows, width), BF16), ((own_rows, columns), F32)],
        [pltpu.VMEM((rows, width), F32)],
    )(at, hidden, chip, chip_got, chip_other, got_other, scale, *summed)
    return (hidden_grad, outproj_grad)


def solution(mesh):
    torus = Mesh(mesh.devices.reshape(4, 2, 4, 2, 2), ("y", "z", "x", "zlo", "core"))
    head = ("zlo", "core")
    return jax.shard_map(
        body,
        mesh=torus,
        in_specs=(
            P(SEQ, None),
            P(SEQ, None),
            P(),
            P(),
            P(),
            P(SEQ, head),
            P(SEQ, head),
            P(SEQ, head),
            P(SEQ, head),
            P(head),
            P(head),
        ),
        out_specs=(P(SEQ, None), P(SEQ, head)),
        check_vma=False,
    )
```
